256 devices in a mesh: rows: 32 (over z, x), tp: 4 (over y), unit: 2 (over core).
Axes of the slice: x: 4, y: 4, z: 8, core: 2. Of those that a mesh axis runs over, the one named last changes fastest.
Arguments:
- train_query: bfloat16 [4096, 2048], P(('unit', 'rows'), 'tp'), parts along dimension 0, may hold values from -0.125 to 0.125
- low_query: bfloat16 [4096, 64], P(('unit', 'rows')), parts along dimension 0, may hold values from -0.125 to 0.125
- high_query: bfloat16 [128, 2048], P('unit', 'tp'), parts along dimension 0, may hold values from -0.75 to 0.75
- train_key: bfloat16 [4096, 512], P(('unit', 'rows'), 'tp'), parts along dimension 0, may hold values from -0.125 to 0.125
- low_key: bfloat16 [4096, 64], P(('unit', 'rows')), parts along dimension 0, may hold values from -0.125 to 0.125
- high_key: bfloat16 [128, 512], P('unit', 'tp'), parts along dimension 0, may hold values from -0.75 to 0.75
- train_value: bfloat16 [4096, 512], P(('unit', 'rows'), 'tp'), parts along dimension 0, may hold values from -0.125 to 0.125
- low_value: bfloat16 [4096, 64], P(('unit', 'rows')), parts along dimension 0, may hold values from -0.125 to 0.125
- high_value: bfloat16 [128, 512], P('unit', 'tp'), parts along dimension 0, may hold values from -0.75 to 0.75
- norm_train: float32 [4096], P(('unit', 'rows', 'tp')), parts along dimension 0, may hold values from 0.25 to 1.75
- norm_step: float32 [4096], P(('unit', 'rows', 'tp')), parts along dimension 0, may hold values from -0.3 to 0.3
Outputs:
- final_query: bfloat16 [4096, 2048], P(('unit', 'tp')), parts along dimension 0
- final_key: bfloat16 [1024, 2048], P(('unit', 'tp')), parts along dimension 0
- final_value: bfloat16 [1024, 2048], P(('unit', 'tp')), parts along dimension 0
- serve_norm: bfloat16 [4096], P('unit'), parts along dimension 0
The draws below stay inside these ranges and needn't reach their ends.
There are 2 independent parts, one for each index of `unit`. The reference program is written for one: setup_inputs(seed, part) draws one part's arguments, and reference() takes and returns one part's arrays. A program takes and returns all parts, laid end to end along the dimension named above; each array names one. Nothing has to cross between parts.
All inputs are finite; a program needn't handle non-finite values.
Results may differ from the reference program's by a relative error of at most 0.001.
Values may be sent and summed in bfloat16 or wider, within the bound.
No kernel may reach another device: no remote copies, remote signals or barrier semaphores. Data moves between devices by JAX's collectives and lax.ppermute only.
A program may use at most 64 MiB of HBM per device.

```python
import jax
import jax.numpy as jnp

D_MODEL = 2048
Q_DIM = 2048
KV_DIM = 512
RANK = 64


def block_levels(key, dims, split, least, largest):
    def one(axis_at, blocks):
        heights = jax.random.uniform(jax.random.fold_in(jax.random.fold_in(key, 6), axis_at), (blocks,), jnp.float32, least / len(split), largest / len(split))
        return jnp.repeat(jnp.exp(heights), dims[axis_at] // blocks).reshape((-1,) + (1,) * (len(dims) - axis_at - 1))

    gain = one(*split[0])
    for cut in split[1:]:
        gain = gain * one(*cut)
    return gain


def scatter_about(key, shape, scale, bound, cuts=(), kind=jnp.bfloat16):
    result = jax.random.normal(key, shape, jnp.float32) * scale
    if len(cuts) > 0:
        result = block_levels(key, shape, cuts, -0.22, 0.18) * result
    return jnp.clip(result, min=-bound, max=bound).astype(kind)


def setup_inputs(seed: int = 0, part: int = 0) -> dict:
    streams_of = jax.random.split(jax.random.key(seed), 12)
    own_keys = jax.random.split(jax.random.fold_in(streams_of[11], part), 12)
    return {
        "train_query": scatter_about(own_keys[0], (D_MODEL, Q_DIM), D_MODEL ** -0.5, 0.125, ((0, 32), (1, 4))),
        "low_query": scatter_about(own_keys[1], (D_MODEL, RANK), D_MODEL ** -0.5, 0.125, ((0, 32),)),
        "high_query": scatter_about(own_keys[2], (RANK, Q_DIM), RANK ** -0.5, 0.75, ((1, 4),)),
        "train_key": scatter_about(own_keys[3], (D_MODEL, KV_DIM), D_MODEL ** -0.5, 0.125, ((0, 32), (1, 4))),
        "low_key": scatter_about(own_keys[4], (D_MODEL, RANK), D_MODEL ** -0.5, 0.125, ((0, 32),)),
        "high_key": scatter_about(own_keys[5], (RANK, KV_DIM), RANK ** -0.5, 0.75, ((1, 4),)),
        "train_value": scatter_about(own_keys[6], (D_MODEL, KV_DIM), D_MODEL ** -0.5, 0.125, ((0, 32), (1, 4))),
        "low_value": scatter_about(own_keys[7], (D_MODEL, RANK), D_MODEL ** -0.5, 0.125, ((0, 32),)),
        "high_value": scatter_about(own_keys[8], (RANK, KV_DIM), RANK ** -0.5, 0.75, ((1, 4),)),
        "norm_train": jnp.clip(1.0 + 0.15 * jax.random.normal(own_keys[9], (D_MODEL,), jnp.float32), 0.25, 1.75),
        "norm_step": jnp.clip(jax.random.uniform(own_keys[10], (D_MODEL,), jnp.float32, -0.3, 0.3) * block_levels(own_keys[10], (D_MODEL,), ((0, 128),), -0.4, 0.0), -0.3, 0.3),
    }


mix_rate = 0.5


def reference(train_query, low_query, high_query, train_key, low_key, high_key, train_value, low_value, high_value, norm_train, norm_step):
    result_query = train_query.astype(jnp.float32) + mix_rate * jnp.dot(low_query, high_query, preferred_element_type=jnp.float32)
    result_key = train_key.astype(jnp.float32) + mix_rate * jnp.dot(low_key, high_key, preferred_element_type=jnp.float32)
    result_value = train_value.astype(jnp.float32) + mix_rate * jnp.dot(low_value, high_value, preferred_element_type=jnp.float32)
    final_query = result_query.T.astype(jnp.bfloat16)
    final_key = result_key.T.astype(jnp.bfloat16)
    final_value = result_value.T.astype(jnp.bfloat16)
    serve_norm = (norm_train + norm_step).astype(jnp.bfloat16)
    return final_query, final_key, final_value, serve_norm
```

```python
import jax
import jax.numpy as jnp
from jax import lax
from jax.experimental import pallas as pl
from jax.experimental.pallas import tpu as pltpu
from jax.sharding import Mesh
from jax.sharding import PartitionSpec as P

ROWS = ("rows_0", "rows_1")
UNIT_ROWS = ("unit", "rows_0", "rows_1")
UNIT_ROWS_TP = ("unit", "rows_0", "rows_1", "tp")
RING_0, RING_1, TP = 8, 4, 4
RANKS = RING_0 * RING_1

mix_rate = 0.5

LANES = 128
BLOCK = 64
CHUNKS = 6
WEIGHT_ROWS = CHUNKS * BLOCK
SENT_ROWS = WEIGHT_ROWS + 8
HALF_ROWS = WEIGHT_ROWS // 2

FAR = ((0, 1), (0, 2), (2, 3), (6, 3), (3, 1), (5, 1), (4, 3))
ALL, LOW, HIGH = (0, CHUNKS), (0, CHUNKS // 2), (CHUNKS // 2, CHUNKS)
NEAR = {
    (1, 0): (((0, 0), ALL), ((0, 1), ALL), ((0, 2), ALL), ((4, 3), ALL), ((5, 1), ALL), ((6, 3), ALL), ((3, 1), HIGH)),
    (-1, 0): (((0, 0), ALL), ((0, 1), ALL), ((0, 2), ALL), ((2, 3), ALL), ((3, 1), ALL), ((4, 3), ALL), ((5, 1), LOW)),
    (0, 1): (((0, 2), ALL), ((2, 3), ALL), ((3, 1), ALL), ((4, 3), ALL), ((5, 1), ALL), ((6, 3), ALL)),
    (0, -1): (((2, 3), ALL), ((3, 1), ALL), ((4, 3), ALL), ((5, 1), ALL), ((6, 3), ALL)),
}


def rows_of(chunks):
    first, last = chunks
    return first * BLOCK, SENT_ROWS if last == CHUNKS else last * BLOCK


def from_offset(array, dz, dx):
    pairs = []
    for z in range(RING_0):
        for x in range(RING_1):
            source = (z + dz) % RING_0 * RING_1 + (x + dx) % RING_1
            pairs.append((source, z * RING_1 + x))
    return lax.ppermute(array, ROWS, pairs)


def merge_kernel(tq, lq, hq, tk, lk, hk, tv, lv, hv, out):
    chunk = 0
    for train, low, high in ((tq, lq, hq), (tk, lk, hk), (tv, lv, hv)):
        result = train[...].astype(jnp.float32) + mix_rate * jnp.dot(
            low[...], high[...], preferred_element_type=jnp.float32
        )
        result = result.astype(jnp.bfloat16)
        for at in range(0, result.shape[1], LANES):
            out[chunk * BLOCK : (chunk + 1) * BLOCK, :] = result[:, at : at + LANES]
            chunk += 1


def place_kernel(pieces, *refs):
    n = len({p[0] for p in pieces})
    sent, (query, key, value, norm), (rows, tiles, turned, sems) = refs[:n], refs[n : n + 4], refs[n + 4 :]
    z, x = lax.axis_index("rows_0"), lax.axis_index("rows_1")
    for at, first_row, (first, last), (dz, dx) in pieces:
        rank = lax.rem(z + dz % RING_0, RING_0) * RING_1 + lax.rem(x + dx % RING_1, RING_1)
        start = pl.multiple_of(rank * BLOCK, BLOCK)
        for chunk in range(first, last):
            row = first_row + (chunk - first) * BLOCK
            rows[chunk, pl.ds(start, BLOCK), :] = sent[at][row : row + BLOCK, :]
        if last == CHUNKS:
            row = first_row + (last - first) * BLOCK
            tiles[rank] = sent[at][row : row + 8, :].astype(jnp.float32)
    lane = lax.broadcasted_iota(jnp.int32, (1, LANES), 1)
    for pair in range(RANKS // 2):
        both = jnp.where(lane < BLOCK, tiles[2 * pair, 0:1, :], tiles[2 * pair + 1, 0:1, :])
        norm[pair : pair + 1, :] = both.astype(jnp.bfloat16)
    copies = []
    for chunk in range(CHUNKS):
        for tile in range(RANKS * BLOCK // LANES):
            lanes = slice(tile * LANES, (tile + 1) * LANES)
            turned[chunk, :, lanes] = rows[chunk, lanes, :].T
        out, row = ((query, chunk), (key, chunk - 4), (value, chunk - 5))[max(0, chunk - 3)]
        copies.append(
            pltpu.make_async_copy(turned.at[chunk], out.at[row * LANES : (row + 1) * LANES, :], sems.at[chunk])
        )
        copies[-1].start()
    for copy in copies:
        copy.wait()


def shards(
    train_query,
    low_query,
    high_query,
    train_key,
    low_key,
    high_key,
    train_value,
    low_value,
    high_value,
    norm_train,
    norm_step,
):
    bf16, vmem = jnp.bfloat16, pl.BlockSpec(memory_space=pltpu.VMEM)
    gain = jnp.tile((norm_train + norm_step).astype(bf16), LANES // 16)
    own = lax.broadcasted_iota(jnp.int32, (8, LANES), 1) // 16 % TP == lax.axis_index("tp")
    gain = jnp.where(own, gain[None, :], jnp.zeros((), bf16))
    others = [lax.ppermute(gain, "tp", [(i, (i + s) % TP) for i in range(TP)]) for s in range(1, TP)]
    merged = pl.pallas_call(
        merge_kernel,
        out_shape=jax.ShapeDtypeStruct((WEIGHT_ROWS, LANES), bf16),
        in_specs=[vmem] * 9,
        out_specs=vmem,
        name="merge",
    )(train_query, low_query, high_query, train_key, low_key, high_key, train_value, low_value, high_value)
    block = jnp.concatenate((merged, gain + others[0] + others[1] + others[2]), axis=0)

    blocks = {(0, 0): block}
    for dz, dx in FAR:
        blocks[dz, dx] = from_offset(block, dz, dx)
    sent, pieces = [], []
    for offset, array in blocks.items():
        pieces.append((len(sent), 0, ALL, offset))
        sent.append(array)
    for (dz, dx), passed in NEAR.items():
        parts, row = [], 0
        for offset, chunks in passed:
            first, last = rows_of(chunks)
            parts.append(blocks[offset][first:last])
            pieces.append((len(sent), row, chunks, (dz + offset[0], dx + offset[1])))
            row += last - first
        sent.append(from_offset(jnp.concatenate(parts, axis=0), dz, dx))

    hbm = pl.BlockSpec(memory_space=pl.ANY)
    width = RANKS * BLOCK
    query, key, value, norm = pl.pallas_call(
        lambda *refs: place_kernel(pieces, *refs),
        out_shape=(
            jax.ShapeDtypeStruct((4 * LANES, width), bf16),
            jax.ShapeDtypeStruct((LANES, width), bf16),
            jax.ShapeDtypeStruct((LANES, width), bf16),
            jax.ShapeDtypeStruct((RANKS // 2, LANES), bf16),
        ),
        in_specs=[vmem] * len(sent),
        out_specs=(hbm, hbm, hbm, vmem),
        scratch_shapes=[
            pltpu.VMEM((CHUNKS, width, LANES), bf16),
            pltpu.VMEM((RANKS, 8, LANES), jnp.float32),
            pltpu.VMEM((CHUNKS, LANES, width), bf16),
            pltpu.SemaphoreType.DMA((CHUNKS,)),
        ],
        name="place",
    )(*sent)
    return query, key, value, norm.reshape(width)


def solution(mesh):
    split = Mesh(
        mesh.devices.reshape(RING_0, RING_1, mesh.shape["tp"], mesh.shape["unit"]),
        ("rows_0", "rows_1", "tp", "unit"),
    )
    return jax.shard_map(
        shards,
        mesh=split,
        in_specs=(
            P(UNIT_ROWS, "tp"),
            P(UNIT_ROWS, None),
            P("unit", "tp"),
            P(UNIT_ROWS, "tp"),
            P(UNIT_ROWS, None),
            P("unit", "tp"),
            P(UNIT_ROWS, "tp"),
            P(UNIT_ROWS, None),
            P("unit", "tp"),
            P(UNIT_ROWS_TP),
            P(UNIT_ROWS_TP),
        ),
        out_specs=(
            P(("unit", "tp"), None),
            P(("unit", "tp"), None),
            P(("unit", "tp"), None),
            P("unit"),
        ),
        check_vma=False,
    )
```

```python
import jax
import jax.numpy as jnp
from jax import lax
from jax.experimental import pallas as pl
from jax.experimental.pallas import tpu as pltpu
from jax.sharding import Mesh
from jax.sharding import PartitionSpec as P

ROWS = ("rows_0", "rows_1")
UNIT_ROWS = ("unit", "rows_0", "rows_1")
UNIT_ROWS_TP = ("unit", "rows_0", "rows_1", "tp")
RING_0, RING_1, TP = 8, 4, 4
RANKS = RING_0 * RING_1

mix_rate = 0.5

LANES = 128
BLOCK = 64
CHUNKS = 6
WEIGHT_ROWS = CHUNKS * BLOCK
SENT_ROWS = WEIGHT_ROWS + 8

FAR = ((5, 2), (1, 1), (2, 0))
ROUNDS = (
    {
        (1, 0): ((1, 1), (2, 0), (5, 2)),
        (-1, 0): ((0, 0), (2, 0), (5, 2)),
        (0, 1): ((0, 0), (1, 1), (5, 2)),
        (0, -1): ((0, 0), (2, 0), (5, 2)),
    },
    {
        (1, 0): ((3, 0), (5, 1), (5, 3), (6, 2)),
        (-1, 0): ((0, 3), (2, 3), (4, 2), (7, 0)),
        (0, 1): ((2, 1), (3, 0), (4, 2), (7, 0)),
        (0, -1): ((0, 3), (3, 0), (4, 2), (5, 1)),
    },
)


def from_offset(array, dz, dx):
    pairs = []
    for z in range(RING_0):
        for x in range(RING_1):
            source = (z + dz) % RING_0 * RING_1 + (x + dx) % RING_1
            pairs.append((source, z * RING_1 + x))
    return lax.ppermute(array, ROWS, pairs)


def merge_kernel(tq, lq, hq, tk, lk, hk, tv, lv, hv, out):
    chunk = 0
    for train, low, high in ((tq, lq, hq), (tk, lk, hk), (tv, lv, hv)):
        result = train[...].astype(jnp.float32) + mix_rate * jnp.dot(
            low[...], high[...], preferred_element_type=jnp.float32
        )
        result = result.astype(jnp.bfloat16)
        for at in range(0, result.shape[1], LANES):
            out[chunk * BLOCK : (chunk + 1) * BLOCK, :] = result[:, at : at + LANES]
            chunk += 1
    out[WEIGHT_ROWS:, :] = jnp.zeros((SENT_ROWS - WEIGHT_ROWS, LANES), jnp.bfloat16)


def gain_kernel(_, own, first, second, third, out):
    out[WEIGHT_ROWS:, :] = own[...] + first[...] + second[...] + third[...]


def place_kernel(pieces, *refs):
    n = 1 + max(p[0] for p in pieces)
    sent, (query, key, value, norm), (rows, tiles, turned, sems) = refs[:n], refs[n : n + 4], refs[n + 4 :]
    z, x = lax.axis_index("rows_0"), lax.axis_index("rows_1")
    for at, row, (dz, dx) in pieces:
        rank = lax.rem(z + dz % RING_0, RING_0) * RING_1 + lax.rem(x + dx % RING_1, RING_1)
        start = pl.multiple_of(rank * BLOCK, BLOCK)
        for chunk in range(CHUNKS):
            rows[chunk, pl.ds(start, BLOCK), :] = sent[at][row + chunk * BLOCK : row + (chunk + 1) * BLOCK, :]
        tiles[rank] = sent[at][row + WEIGHT_ROWS : row + SENT_ROWS, :].astype(jnp.float32)
    lane = lax.broadcasted_iota(jnp.int32, (1, LANES), 1)
    for pair in range(RANKS // 2):
        both = jnp.where(lane < BLOCK, tiles[2 * pair, 0:1, :], tiles[2 * pair + 1, 0:1, :])
        norm[pair : pair + 1, :] = both.astype(jnp.bfloat16)
    copies = []
    for chunk in range(CHUNKS):
        for tile in range(RANKS * BLOCK // LANES):
            lanes = slice(tile * LANES, (tile + 1) * LANES)
            turned[chunk, :, lanes] = rows[chunk, lanes, :].T
        out, row = ((query, chunk), (key, chunk - 4), (value, chunk - 5))[max(0, chunk - 3)]
        copies.append(
            pltpu.make_async_copy(turned.at[chunk], out.at[row * LANES : (row + 1) * LANES, :], sems.at[chunk])
        )
        copies[-1].start()
    for copy in copies:
        copy.wait()


def shards(
    train_query,
    low_query,
    high_query,
    train_key,
    low_key,
    high_key,
    train_value,
    low_value,
    high_value,
    norm_train,
    norm_step,
):
    bf16, vmem = jnp.bfloat16, pl.BlockSpec(memory_space=pltpu.VMEM)
    gain = jnp.tile((norm_train + norm_step).astype(bf16), LANES // 16)
    own = lax.broadcasted_iota(jnp.int32, (8, LANES), 1) // 16 % TP == lax.axis_index("tp")
    gain = jnp.where(own, gain[None, :], jnp.zeros((), bf16))
    others = [lax.ppermute(gain, "tp", [(i, (i + s) % TP) for i in range(TP)]) for s in range(1, TP)]
    block = pl.pallas_call(
        merge_kernel,
        out_shape=pltpu.VMEM((SENT_ROWS, LANES), bf16),
        in_specs=[vmem] * 9,
        out_specs=vmem,
        name="merge",
    )(train_query, low_query, high_query, train_key, low_key, high_key, train_value, low_value, high_value)
    block = pl.pallas_call(
        gain_kernel,
        out_shape=pltpu.VMEM((SENT_ROWS, LANES), bf16),
        in_specs=[vmem] * 5,
        out_specs=vmem,
        input_output_aliases={0: 0},
        name="gain",
    )(*(pltpu.with_memory_space_constraint(a, pltpu.VMEM) for a in (block, gain, *others)))

    sent, pieces = [block], [(0, 0, (0, 0))]
    for offset in FAR:
        pieces.append((len(sent), 0, offset))
        sent.append(from_offset(block, *offset))
    for passed in ROUNDS:
        held = {(dz % RING_0, dx % RING_1): (at, row) for at, row, (dz, dx) in pieces}
        payloads = {
            offsets: jnp.concatenate([sent[at][row : row + SENT_ROWS] for at, row in (held[o] for o in offsets)], axis=0)
            for offsets in passed.values()
        }
        for (dz, dx), offsets in passed.items():
            for number, offset in enumerate(offsets):
                pieces.append((len(sent), number * SENT_ROWS, (dz + offset[0], dx + offset[1])))
            sent.append(from_offset(payloads[offsets], dz, dx))

    hbm = pl.BlockSpec(memory_space=pl.ANY)
    width = RANKS * BLOCK
    query, key, value, norm = pl.pallas_call(
        lambda *refs: place_kernel(pieces, *refs),
        out_shape=(
            jax.ShapeDtypeStruct((4 * LANES, width), bf16),
            jax.ShapeDtypeStruct((LANES, width), bf16),
            jax.ShapeDtypeStruct((LANES, width), bf16),
            jax.ShapeDtypeStruct((RANKS // 2, LANES), bf16),
        ),
        in_specs=[vmem] * len(sent),
        out_specs=(hbm, hbm, hbm, vmem),
        scratch_shapes=[
            pltpu.VMEM((CHUNKS, width, LANES), bf16),
            pltpu.VMEM((RANKS, 8, LANES), jnp.float32),
            pltpu.VMEM((CHUNKS, LANES, width), bf16),
            pltpu.SemaphoreType.DMA((CHUNKS,)),
        ],
        compiler_params=pltpu.CompilerParams(vmem_limit_bytes=16 * 2**20),
        name="place",
    )(*(pltpu.with_memory_space_constraint(a, pltpu.VMEM) for a in sent))
    return query, key, value, norm.reshape(width)


def solution(mesh):
    split = Mesh(
        mesh.devices.reshape(RING_0, RING_1, mesh.shape["tp"], mesh.shape["unit"]),
        ("rows_0", "rows_1", "tp", "unit"),
    )
    return jax.shard_map(
        shards,
        mesh=split,
        in_specs=(
            P(UNIT_ROWS, "tp"),
            P(UNIT_ROWS, None),
            P("unit", "tp"),
            P(UNIT_ROWS, "tp"),
            P(UNIT_ROWS, None),
            P("unit", "tp"),
            P(UNIT_ROWS, "tp"),
            P(UNIT_ROWS, None),
            P("unit", "tp"),
            P(UNIT_ROWS_TP),
            P(UNIT_ROWS_TP),
        ),
        out_specs=(
            P(("unit", "tp"), None),
            P(("unit", "tp"), None),
            P(("unit", "tp"), None),
            P("unit"),
        ),
        check_vma=False,
    )
```

```python
import jax
import jax.numpy as jnp
from jax import lax
from jax.experimental import pallas as pl
from jax.experimental.pallas import tpu as pltpu
from jax.sharding import Mesh
from jax.sharding import PartitionSpec as P

ROWS = ("rows_0", "rows_1")
UNIT_ROWS = ("unit", "rows_0", "rows_1")
UNIT_ROWS_TP = ("unit", "rows_0", "rows_1", "tp")
RING_0, RING_1, TP = 8, 4, 4
RANKS = RING_0 * RING_1

mix_rate = 0.5

LANES = 128
BLOCK = 64
CHUNKS = 6
WEIGHT_ROWS = CHUNKS * BLOCK
SENT_ROWS = WEIGHT_ROWS + 8

STEPS = (
    ((4, 0), ((0, 0),)),
    ((0, 2), ((0, 0),)),
    ((2, 0), ((0, 0),)),
    ((6, 0), ((0, 0),)),
    ((-1, 0), ((0, 0), (0, 2))),
    ((0, -1), ((4, 0),)),
    ((1, 0), ((0, 0), (0, 2), (4, 0))),
    ((0, 1), ((4, 0),)),
    ((0, -1), ((2, 0), (4, 3))),
    ((0, 1), ((0, 0), (2, 0), (6, 0))),
    ((-1, 0), ((4, 1), (4, 3))),
    ((1, 0), ((2, 0), (4, 3))),
    ((0, -1), ((0, 0), (6, 0), (7, 2), (7, 0))),
    ((-1, 0), ((2, 3), (4, 2), (7, 2))),
    ((0, 1), ((1, 0), (5, 0))),
    ((1, 0), ((1, 2), (4, 2))),
)


def from_offset(array, dz, dx):
    pairs = []
    for z in range(RING_0):
        for x in range(RING_1):
            source = (z + dz) % RING_0 * RING_1 + (x + dx) % RING_1
            pairs.append((source, z * RING_1 + x))
    return lax.ppermute(array, ROWS, pairs)


def merge_kernel(tq, lq, hq, tk, lk, hk, tv, lv, hv, out):
    chunk = 0
    for train, low, high in ((tq, lq, hq), (tk, lk, hk), (tv, lv, hv)):
        result = train[...].astype(jnp.float32) + mix_rate * jnp.dot(
            low[...], high[...], preferred_element_type=jnp.float32
        )
        result = result.astype(jnp.bfloat16)
        for at in range(0, result.shape[1], LANES):
            out[chunk * BLOCK : (chunk + 1) * BLOCK, :] = result[:, at : at + LANES]
            chunk += 1
    out[WEIGHT_ROWS:, :] = jnp.zeros((SENT_ROWS - WEIGHT_ROWS, LANES), jnp.bfloat16)


def gain_kernel(_, own, first, second, third, out):
    out[WEIGHT_ROWS:, :] = own[...] + first[...] + second[...] + third[...]


def place_kernel(pieces, *refs):
    n = 1 + max(p[0] for p in pieces)
    sent, (query, key, value, norm), (rows, tiles, turned, sems) = refs[:n], refs[n : n + 4], refs[n + 4 :]
    z, x = lax.axis_index("rows_0"), lax.axis_index("rows_1")
    for at, row, (dz, dx) in pieces:
        rank = lax.rem(z + dz % RING_0, RING_0) * RING_1 + lax.rem(x + dx % RING_1, RING_1)
        start = pl.multiple_of(rank * BLOCK, BLOCK)
        for chunk in range(CHUNKS):
            rows[chunk, pl.ds(start, BLOCK), :] = sent[at][row + chunk * BLOCK : row + (chunk + 1) * BLOCK, :]
        tiles[rank] = sent[at][row + WEIGHT_ROWS : row + SENT_ROWS, :].astype(jnp.float32)
    lane = lax.broadcasted_iota(jnp.int32, (1, LANES), 1)
    for pair in range(RANKS // 2):
        both = jnp.where(lane < BLOCK, tiles[2 * pair, 0:1, :], tiles[2 * pair + 1, 0:1, :])
        norm[pair : pair + 1, :] = both.astype(jnp.bfloat16)
    copies = []
    for chunk in range(CHUNKS):
        for tile in range(RANKS * BLOCK // LANES):
            lanes = slice(tile * LANES, (tile + 1) * LANES)
            turned[chunk, :, lanes] = rows[chunk, lanes, :].T
        out, row = ((query, chunk), (key, chunk - 4), (value, chunk - 5))[max(0, chunk - 3)]
        copies.append(
            pltpu.make_async_copy(turned.at[chunk], out.at[row * LANES : (row + 1) * LANES, :], sems.at[chunk])
        )
        copies[-1].start()
    for copy in copies:
        copy.wait()


def shards(
    train_query,
    low_query,
    high_query,
    train_key,
    low_key,
    high_key,
    train_value,
    low_value,
    high_value,
    norm_train,
    norm_step,
):
    bf16, vmem = jnp.bfloat16, pl.BlockSpec(memory_space=pltpu.VMEM)
    gain = jnp.tile((norm_train + norm_step).astype(bf16), LANES // 16)
    own = lax.broadcasted_iota(jnp.int32, (8, LANES), 1) // 16 % TP == lax.axis_index("tp")
    gain = jnp.where(own, gain[None, :], jnp.zeros((), bf16))
    others = [lax.ppermute(gain, "tp", [(i, (i + s) % TP) for i in range(TP)]) for s in range(1, TP)]
    block = pl.pallas_call(
        merge_kernel,
        out_shape=pltpu.VMEM((SENT_ROWS, LANES), bf16),
        in_specs=[vmem] * 9,
        out_specs=vmem,
        name="merge",
    )(train_query, low_query, high_query, train_key, low_key, high_key, train_value, low_value, high_value)
    block = pl.pallas_call(
        gain_kernel,
        out_shape=pltpu.VMEM((SENT_ROWS, LANES), bf16),
        in_specs=[vmem] * 5,
        out_specs=vmem,
        input_output_aliases={0: 0},
        name="gain",
    )(*(pltpu.with_memory_space_constraint(a, pltpu.VMEM) for a in (block, gain, *others)))

    sent, held = [block], {(0, 0): (0, 0)}
    for offset, passed in STEPS:
        parts = [sent[at][row : row + SENT_ROWS] for at, row in (held[p] for p in passed)]
        arrived = from_offset(parts[0] if len(parts) == 1 else jnp.concatenate(parts, axis=0), *offset)
        for place, (dz, dx) in enumerate(passed):
            held[(offset[0] + dz) % RING_0, (offset[1] + dx) % RING_1] = (len(sent), place * SENT_ROWS)
        sent.append(arrived)
    pieces = [(at, row, offset) for offset, (at, row) in held.items()]
    assert len(pieces) == RANKS == 1 + sum(len(passed) for _, passed in STEPS)

    hbm = pl.BlockSpec(memory_space=pl.ANY)
    width = RANKS * BLOCK
    query, key, value, norm = pl.pallas_call(
        lambda *refs: place_kernel(pieces, *refs),
        out_shape=(
            jax.ShapeDtypeStruct((4 * LANES, width), bf16),
            jax.ShapeDtypeStruct((LANES, width), bf16),
            jax.ShapeDtypeStruct((LANES, width), bf16),
            jax.ShapeDtypeStruct((RANKS // 2, LANES), bf16),
        ),
        in_specs=[vmem] * len(sent),
        out_specs=(hbm, hbm, hbm, vmem),
        scratch_shapes=[
            pltpu.VMEM((CHUNKS, width, LANES), bf16),
            pltpu.VMEM((RANKS, 8, LANES), jnp.float32),
            pltpu.VMEM((CHUNKS, LANES, width), bf16),
            pltpu.SemaphoreType.DMA((CHUNKS,)),
        ],
        compiler_params=pltpu.CompilerParams(vmem_limit_bytes=16 * 2**20),
        name="place",
    )(*(pltpu.with_memory_space_constraint(a, pltpu.VMEM) for a in sent))
    return query, key, value, norm.reshape(width)


def solution(mesh):
    split = Mesh(
        mesh.devices.reshape(RING_0, RING_1, mesh.shape["tp"], mesh.shape["unit"]),
        ("rows_0", "rows_1", "tp", "unit"),
    )
    return jax.shard_map(
        shards,
        mesh=split,
        in_specs=(
            P(UNIT_ROWS, "tp"),
            P(UNIT_ROWS, None),
            P("unit", "tp"),
            P(UNIT_ROWS, "tp"),
            P(UNIT_ROWS, None),
            P("unit", "tp"),
            P(UNIT_ROWS, "tp"),
            P(UNIT_ROWS, None),
            P("unit", "tp"),
            P(UNIT_ROWS_TP),
            P(UNIT_ROWS_TP),
        ),
        out_specs=(
            P(("unit", "tp"), None),
            P(("unit", "tp"), None),
            P(("unit", "tp"), None),
            P("unit"),
        ),
        check_vma=False,
    )
```

```python
import jax
import jax.numpy as jnp
from jax import lax
from jax.experimental import pallas as pl
from jax.experimental.pallas import tpu as pltpu
from jax.sharding import Mesh
from jax.sharding import PartitionSpec as P

ROWS = ("rows_0", "rows_1")
UNIT_ROWS = ("unit", "rows_0", "rows_1")
UNIT_ROWS_TP = ("unit", "rows_0", "rows_1", "tp")
RING_0, RING_1, TP = 8, 4, 4
RANKS = RING_0 * RING_1

mix_rate = 0.5

LANES = 128
BLOCK = 64
CHUNKS = 6
WEIGHT_ROWS = CHUNKS * BLOCK
SENT_ROWS = WEIGHT_ROWS + 8

STEPS = (
    ((4, 0), ((0, 0),)),
    ((7, 0), ((0, 0),)),
    ((2, 2), ((0, 0),)),
    ((6, 2), ((0, 0),)),
    ((1, 0), ((0, 0), (4, 0))),
    ((0, 1), ((0, 0), (4, 0))),
    ((0, -1), ((2, 2), (4, 0))),
    ((-1, 0), ((2, 2), (4, 0), (7, 0))),
    ((0, -1), ((0, 0), (1, 0), (5, 0), (6, 2), (7, 0))),
    ((0, 1), ((0, 1), (2, 2), (4, 1), (6, 2), (7, 0))),
    ((1, 0), ((1, 0), (2, 2), (4, 1), (6, 2))),
    ((-1, 0), ((2, 1), (4, 1), (4, 3), (6, 2))),
)


def from_offset(array, dz, dx):
    pairs = []
    for z in range(RING_0):
        for x in range(RING_1):
            source = (z + dz) % RING_0 * RING_1 + (x + dx) % RING_1
            pairs.append((source, z * RING_1 + x))
    return lax.ppermute(array, ROWS, pairs)


def merge_kernel(tq, lq, hq, tk, lk, hk, tv, lv, hv, out):
    chunk = 0
    for train, low, high in ((tq, lq, hq), (tk, lk, hk), (tv, lv, hv)):
        result = train[...].astype(jnp.float32) + mix_rate * jnp.dot(
            low[...], high[...], preferred_element_type=jnp.float32
        )
        result = result.astype(jnp.bfloat16)
        for at in range(0, result.shape[1], LANES):
            out[chunk * BLOCK : (chunk + 1) * BLOCK, :] = result[:, at : at + LANES]
            chunk += 1
    out[WEIGHT_ROWS:, :] = jnp.zeros((SENT_ROWS - WEIGHT_ROWS, LANES), jnp.bfloat16)


def gain_kernel(_, own, first, second, third, out):
    out[WEIGHT_ROWS:, :] = own[...] + first[...] + second[...] + third[...]


def pack(sent, parts):
    if len(parts) == 1 and sent[parts[0][0]].shape[0] == SENT_ROWS:
        return sent[parts[0][0]]
    used = sorted({at for at, _ in parts})

    def kernel(*refs):
        for number, (at, row) in enumerate(parts):
            to = number * SENT_ROWS
            refs[-1][to : to + SENT_ROWS, :] = refs[used.index(at)][row : row + SENT_ROWS, :]

    vmem = pl.BlockSpec(memory_space=pltpu.VMEM)
    return pl.pallas_call(
        kernel,
        out_shape=pltpu.VMEM((len(parts) * SENT_ROWS, LANES), jnp.bfloat16),
        in_specs=[vmem] * len(used),
        out_specs=vmem,
        compiler_params=pltpu.CompilerParams(vmem_limit_bytes=2**20),
        name="pack",
    )(*(pltpu.with_memory_space_constraint(sent[at], pltpu.VMEM) for at in used))


def place_kernel(pieces, *refs):
    n = 1 + max(p[0] for p in pieces)
    sent, (query, key, value, norm), (rows, tiles, turned, sems) = refs[:n], refs[n : n + 4], refs[n + 4 :]
    z, x = lax.axis_index("rows_0"), lax.axis_index("rows_1")
    for at, row, (dz, dx) in pieces:
        rank = lax.rem(z + dz % RING_0, RING_0) * RING_1 + lax.rem(x + dx % RING_1, RING_1)
        start = pl.multiple_of(rank * BLOCK, BLOCK)
        for chunk in range(CHUNKS):
            rows[chunk, pl.ds(start, BLOCK), :] = sent[at][row + chunk * BLOCK : row + (chunk + 1) * BLOCK, :]
        tiles[rank] = sent[at][row + WEIGHT_ROWS : row + SENT_ROWS, :].astype(jnp.float32)
    lane = lax.broadcasted_iota(jnp.int32, (1, LANES), 1)
    for pair in range(RANKS // 2):
        both = jnp.where(lane < BLOCK, tiles[2 * pair, 0:1, :], tiles[2 * pair + 1, 0:1, :])
        norm[pair : pair + 1, :] = both.astype(jnp.bfloat16)
    copies = []
    for chunk in range(CHUNKS):
        for tile in range(RANKS * BLOCK // LANES):
            lanes = slice(tile * LANES, (tile + 1) * LANES)
            turned[chunk, :, lanes] = rows[chunk, lanes, :].T
        out, row = ((query, chunk), (key, chunk - 4), (value, chunk - 5))[max(0, chunk - 3)]
        copies.append(
            pltpu.make_async_copy(turned.at[chunk], out.at[row * LANES : (row + 1) * LANES, :], sems.at[chunk])
        )
        copies[-1].start()
    for copy in copies:
        copy.wait()


def shards(
    train_query,
    low_query,
    high_query,
    train_key,
    low_key,
    high_key,
    train_value,
    low_value,
    high_value,
    norm_train,
    norm_step,
):
    bf16, vmem = jnp.bfloat16, pl.BlockSpec(memory_space=pltpu.VMEM)
    gain = jnp.tile((norm_train + norm_step).astype(bf16), LANES // 16)
    own = lax.broadcasted_iota(jnp.int32, (8, LANES), 1) // 16 % TP == lax.axis_index("tp")
    gain = jnp.where(own, gain[None, :], jnp.zeros((), bf16))
    others = [lax.ppermute(gain, "tp", [(i, (i + s) % TP) for i in range(TP)]) for s in range(1, TP)]
    block = pl.pallas_call(
        merge_kernel,
        out_shape=pltpu.VMEM((SENT_ROWS, LANES), bf16),
        in_specs=[vmem] * 9,
        out_specs=vmem,
        name="merge",
    )(train_query, low_query, high_query, train_key, low_key, high_key, train_value, low_value, high_value)
    block = pl.pallas_call(
        gain_kernel,
        out_shape=pltpu.VMEM((SENT_ROWS, LANES), bf16),
        in_specs=[vmem] * 5,
        out_specs=vmem,
        input_output_aliases={0: 0},
        name="gain",
    )(*(pltpu.with_memory_space_constraint(a, pltpu.VMEM) for a in (block, gain, *others)))

    sent, held = [block], {(0, 0): (0, 0)}
    for offset, passed in STEPS:
        arrived = from_offset(pack(sent, [held[p] for p in passed]), *offset)
        for place, (dz, dx) in enumerate(passed):
            held[(offset[0] + dz) % RING_0, (offset[1] + dx) % RING_1] = (len(sent), place * SENT_ROWS)
        sent.append(arrived)
    pieces = [(at, row, offset) for offset, (at, row) in held.items()]
    assert len(pieces) == RANKS == 1 + sum(len(passed) for _, passed in STEPS)

    hbm = pl.BlockSpec(memory_space=pl.ANY)
    width = RANKS * BLOCK
    query, key, value, norm = pl.pallas_call(
        lambda *refs: place_kernel(pieces, *refs),
        out_shape=(
            jax.ShapeDtypeStruct((4 * LANES, width), bf16),
            jax.ShapeDtypeStruct((LANES, width), bf16),
            jax.ShapeDtypeStruct((LANES, width), bf16),
            jax.ShapeDtypeStruct((RANKS // 2, LANES), bf16),
        ),
        in_specs=[vmem] * len(sent),
        out_specs=(hbm, hbm, hbm, vmem),
        scratch_shapes=[
            pltpu.VMEM((CHUNKS, width, LANES), bf16),
            pltpu.VMEM((RANKS, 8, LANES), jnp.float32),
            pltpu.VMEM((CHUNKS, LANES, width), bf16),
            pltpu.SemaphoreType.DMA((CHUNKS,)),
        ],
        compiler_params=pltpu.CompilerParams(vmem_limit_bytes=16 * 2**20),
        name="place",
    )(*(pltpu.with_memory_space_constraint(a, pltpu.VMEM) for a in sent))
    return query, key, value, norm.reshape(width)


def solution(mesh):
    split = Mesh(
        mesh.devices.reshape(RING_0, RING_1, mesh.shape["tp"], mesh.shape["unit"]),
        ("rows_0", "rows_1", "tp", "unit"),
    )
    return jax.shard_map(
        shards,
        mesh=split,
        in_specs=(
            P(UNIT_ROWS, "tp"),
            P(UNIT_ROWS, None),
            P("unit", "tp"),
            P(UNIT_ROWS, "tp"),
            P(UNIT_ROWS, None),
            P("unit", "tp"),
            P(UNIT_ROWS, "tp"),
            P(UNIT_ROWS, None),
            P("unit", "tp"),
            P(UNIT_ROWS_TP),
            P(UNIT_ROWS_TP),
        ),
        out_specs=(
            P(("unit", "tp"), None),
            P(("unit", "tp"), None),
            P(("unit", "tp"), None),
            P("unit"),
        ),
        check_vma=False,
    )
```

```python
import jax
import jax.numpy as jnp
from jax import lax
from jax.experimental import pallas as pl
from jax.experimental.pallas import tpu as pltpu
from jax.sharding import Mesh
from jax.sharding import PartitionSpec as P

ROWS = ("rows_0", "rows_1")
UNIT_ROWS = ("unit", "rows_0", "rows_1")
UNIT_ROWS_TP = ("unit", "rows_0", "rows_1", "tp")
RING_0, RING_1, TP = 8, 4, 4
RANKS = RING_0 * RING_1

mix_rate = 0.5

LANES = 128
BLOCK = 64
CHUNKS = 6
WEIGHT_ROWS = CHUNKS * BLOCK
SENT_ROWS = WEIGHT_ROWS + 8

FIRST, LAST = (0, CHUNKS // 2), (CHUNKS // 2, CHUNKS)
WHOLE = (FIRST, LAST)
STEPS = (
    ((4, 0), ((0, 0, WHOLE),)),
    ((2, 2), ((0, 0, WHOLE),)),
    ((7, 0), ((0, 0, WHOLE),)),
    ((6, 2), ((0, 0, WHOLE),)),
    ((1, 0), ((0, 0, WHOLE),)),
    ((0, -1), ((4, 0, WHOLE), (7, 0, WHOLE),)),
    ((0, 1), ((0, 0, WHOLE), (4, 0, WHOLE),)),
    ((1, 0), ((1, 0, WHOLE), (2, 2, WHOLE), (4, 0, WHOLE),)),
    ((-1, 0), ((2, 2, WHOLE), (4, 0, WHOLE), (7, 0, WHOLE),)),
    ((0, -1), ((0, 0, WHOLE), (1, 0, WHOLE), (2, 2, WHOLE), (4, 3, (LAST,)), (6, 2, WHOLE), (7, 3, (FIRST,)),)),
    ((0, 1), ((0, 1, WHOLE), (2, 2, WHOLE), (4, 1, (FIRST,)), (6, 2, WHOLE), (7, 0, WHOLE),)),
    ((1, 0), ((0, 1, WHOLE), (4, 1, WHOLE), (4, 3, WHOLE), (6, 2, (LAST,)),)),
    ((-1, 0), ((4, 1, WHOLE), (4, 3, WHOLE), (6, 2, WHOLE),)),
)


def from_offset(array, dz, dx):
    pairs = []
    for z in range(RING_0):
        for x in range(RING_1):
            source = (z + dz) % RING_0 * RING_1 + (x + dx) % RING_1
            pairs.append((source, z * RING_1 + x))
    return lax.ppermute(array, ROWS, pairs)


def merge_kernel(tq, lq, hq, tk, lk, hk, tv, lv, hv, out):
    chunk = 0
    for train, low, high in ((tq, lq, hq), (tk, lk, hk), (tv, lv, hv)):
        result = train[...].astype(jnp.float32) + mix_rate * jnp.dot(
            low[...], high[...], preferred_element_type=jnp.float32
        )
        result = result.astype(jnp.bfloat16)
        for at in range(0, result.shape[1], LANES):
            out[chunk * BLOCK : (chunk + 1) * BLOCK, :] = result[:, at : at + LANES]
            chunk += 1
    out[WEIGHT_ROWS:, :] = jnp.zeros((SENT_ROWS - WEIGHT_ROWS, LANES), jnp.bfloat16)


def gain_kernel(_, own, first, second, third, out):
    out[WEIGHT_ROWS:, :] = own[...] + first[...] + second[...] + third[...]


def size_of(half):
    first, last = half
    return (last - first) * BLOCK + (SENT_ROWS - WEIGHT_ROWS if last == CHUNKS else 0)


def pack(sent, parts):
    total = sum(size for _, _, size in parts)
    if len({at for at, _, _ in parts}) == 1 and sent[parts[0][0]].shape[0] == total:
        return sent[parts[0][0]]
    used = sorted({at for at, _, _ in parts})

    def kernel(*refs):
        to = 0
        for at, row, size in parts:
            refs[-1][to : to + size, :] = refs[used.index(at)][row : row + size, :]
            to += size

    vmem = pl.BlockSpec(memory_space=pltpu.VMEM)
    return pl.pallas_call(
        kernel,
        out_shape=pltpu.VMEM((total, LANES), jnp.bfloat16),
        in_specs=[vmem] * len(used),
        out_specs=vmem,
        compiler_params=pltpu.CompilerParams(vmem_limit_bytes=2**20),
        name="pack",
    )(*(pltpu.with_memory_space_constraint(sent[at], pltpu.VMEM) for at in used))


def place_kernel(pieces, *refs):
    n = 1 + max(p[0] for p in pieces)
    sent, (query, key, value, norm), (rows, tiles, turned, sems) = refs[:n], refs[n : n + 4], refs[n + 4 :]
    z, x = lax.axis_index("rows_0"), lax.axis_index("rows_1")
    placed = []
    for at, row, (first, last), (dz, dx) in pieces:
        rank = lax.rem(z + dz, RING_0) * RING_1 + lax.rem(x + dx, RING_1)
        placed.append((sent[at], row, first, last, rank))
    copies = []
    for chunk in range(CHUNKS):
        for block, row, first, last, rank in placed:
            if first <= chunk < last:
                at = row + (chunk - first) * BLOCK
                rows[chunk, pl.ds(pl.multiple_of(rank * BLOCK, BLOCK), BLOCK), :] = block[at : at + BLOCK, :]
        for tile in range(RANKS * BLOCK // LANES):
            lanes = slice(tile * LANES, (tile + 1) * LANES)
            turned[chunk, :, lanes] = rows[chunk, lanes, :].T
        out, row = ((query, chunk), (key, chunk - 4), (value, chunk - 5))[max(0, chunk - 3)]
        copies.append(
            pltpu.make_async_copy(turned.at[chunk], out.at[row * LANES : (row + 1) * LANES, :], sems.at[chunk])
        )
        copies[-1].start()
    for block, row, first, last, rank in placed:
        if last == CHUNKS:
            at = row + (last - first) * BLOCK
            tiles[rank] = block[at : at + 8, :].astype(jnp.float32)
    lane = lax.broadcasted_iota(jnp.int32, (1, LANES), 1)
    for pair in range(RANKS // 2):
        both = jnp.where(lane < BLOCK, tiles[2 * pair, 0:1, :], tiles[2 * pair + 1, 0:1, :])
        norm[pair : pair + 1, :] = both.astype(jnp.bfloat16)
    for copy in copies:
        copy.wait()


def shards(
    train_query,
    low_query,
    high_query,
    train_key,
    low_key,
    high_key,
    train_value,
    low_value,
    high_value,
    norm_train,
    norm_step,
):
    bf16, vmem = jnp.bfloat16, pl.BlockSpec(memory_space=pltpu.VMEM)
    gain = jnp.tile((norm_train + norm_step).astype(bf16), LANES // 16)
    own = lax.broadcasted_iota(jnp.int32, (8, LANES), 1) // 16 % TP == lax.axis_index("tp")
    gain = jnp.where(own, gain[None, :], jnp.zeros((), bf16))
    others = [lax.ppermute(gain, "tp", [(i, (i + s) % TP) for i in range(TP)]) for s in range(1, TP)]
    block = pl.pallas_call(
        merge_kernel,
        out_shape=pltpu.VMEM((SENT_ROWS, LANES), bf16),
        in_specs=[vmem] * 9,
        out_specs=vmem,
        name="merge",
    )(train_query, low_query, high_query, train_key, low_key, high_key, train_value, low_value, high_value)
    block = pl.pallas_call(
        gain_kernel,
        out_shape=pltpu.VMEM((SENT_ROWS, LANES), bf16),
        in_specs=[vmem] * 5,
        out_specs=vmem,
        input_output_aliases={0: 0},
        name="gain",
    )(*(pltpu.with_memory_space_constraint(a, pltpu.VMEM) for a in (block, gain, *others)))

    sent = [block]
    held = {(0, 0, FIRST): (0, 0), (0, 0, LAST): (0, size_of(FIRST))}
    for offset, passed in STEPS:
        parts, row = [], 0
        for dz, dx, halves in passed:
            for half in halves:
                at, start = held[dz, dx, half]
                parts.append((at, start, size_of(half)))
                held[(offset[0] + dz) % RING_0, (offset[1] + dx) % RING_1, half] = (len(sent), row)
                row += size_of(half)
        sent.append(from_offset(pack(sent, parts), *offset))
    pieces = [(at, row, half, (dz, dx)) for (dz, dx, half), (at, row) in held.items()]
    assert len(pieces) == 2 * RANKS == 2 + sum(len(halves) for _, passed in STEPS for _, _, halves in passed)

    hbm = pl.BlockSpec(memory_space=pl.ANY)
    width = RANKS * BLOCK
    query, key, value, norm = pl.pallas_call(
        lambda *refs: place_kernel(pieces, *refs),
        out_shape=(
            jax.ShapeDtypeStruct((4 * LANES, width), bf16),
            jax.ShapeDtypeStruct((LANES, width), bf16),
            jax.ShapeDtypeStruct((LANES, width), bf16),
            jax.ShapeDtypeStruct((RANKS // 2, LANES), bf16),
        ),
        in_specs=[vmem] * len(sent),
        out_specs=(hbm, hbm, hbm, vmem),
        scratch_shapes=[
            pltpu.VMEM((CHUNKS, width, LANES), bf16),
            pltpu.VMEM((RANKS, 8, LANES), jnp.float32),
            pltpu.VMEM((CHUNKS, LANES, width), bf16),
            pltpu.SemaphoreType.DMA((CHUNKS,)),
        ],
        compiler_params=pltpu.CompilerParams(vmem_limit_bytes=16 * 2**20),
        name="place",
    )(*(pltpu.with_memory_space_constraint(a, pltpu.VMEM) for a in sent))
    return query, key, value, norm.reshape(width)


def solution(mesh):
    split = Mesh(
        mesh.devices.reshape(RING_0, RING_1, mesh.shape["tp"], mesh.shape["unit"]),
        ("rows_0", "rows_1", "tp", "unit"),
    )
    return jax.shard_map(
        shards,
        mesh=split,
        in_specs=(
            P(UNIT_ROWS, "tp"),
            P(UNIT_ROWS, None),
            P("unit", "tp"),
            P(UNIT_ROWS, "tp"),
            P(UNIT_ROWS, None),
            P("unit", "tp"),
            P(UNIT_ROWS, "tp"),
            P(UNIT_ROWS, None),
            P("unit", "tp"),
            P(UNIT_ROWS_TP),
            P(UNIT_ROWS_TP),
        ),
        out_specs=(
            P(("unit", "tp"), None),
            P(("unit", "tp"), None),
            P(("unit", "tp"), None),
            P("unit"),
        ),
        check_vma=False,
    )
```

```python
import jax
import jax.numpy as jnp
from jax import lax
from jax.experimental import pallas as pl
from jax.experimental.pallas import tpu as pltpu
from jax.sharding import Mesh
from jax.sharding import PartitionSpec as P

ROWS = ("rows_0", "rows_1")
UNIT_ROWS = ("unit", "rows_0", "rows_1")
UNIT_ROWS_TP = ("unit", "rows_0", "rows_1", "tp")
RING_0, RING_1, TP = 8, 4, 4
RANKS = RING_0 * RING_1

mix_rate = 0.5

LANES = 128
BLOCK = 64
CHUNKS = 6
WEIGHT_ROWS = CHUNKS * BLOCK
SENT_ROWS = WEIGHT_ROWS + 8

FIRST, LAST = (0, CHUNKS // 2), (CHUNKS // 2, CHUNKS)
WHOLE = (FIRST, LAST)
STEPS = (
    ((5, 0), ((0, 0, WHOLE),)),
    ((2, 2), ((0, 0, WHOLE),)),
    ((6, 2), ((0, 0, WHOLE),)),
    ((1, 0), ((0, 0, WHOLE),)),
    ((0, 1), ((0, 0, WHOLE),)),
    ((-1, 0), ((5, 0, WHOLE), (0, 0, WHOLE),)),
    ((0, -1), ((0, 0, WHOLE), (2, 2, WHOLE), (5, 0, WHOLE),)),
    ((1, 0), ((1, 0, WHOLE), (2, 2, WHOLE),)),
    ((0, 1), ((0, 1, WHOLE), (2, 2, WHOLE), (5, 0, WHOLE), (6, 2, WHOLE),)),
    ((-1, 0), ((2, 2, WHOLE), (4, 0, WHOLE), (6, 2, WHOLE), (7, 0, WHOLE), (0, 1, WHOLE),)),
    ((0, -1), ((1, 0, WHOLE), (4, 0, WHOLE), (6, 2, WHOLE), (7, 0, WHOLE),)),
    ((1, 0), ((0, 1, (LAST,)), (2, 1, WHOLE), (3, 2, WHOLE), (6, 2, WHOLE),)),
    ((0, 1), ((1, 0, (FIRST,)), (3, 2, WHOLE), (4, 0, WHOLE),)),
)


def from_offset(array, dz, dx):
    pairs = []
    for z in range(RING_0):
        for x in range(RING_1):
            source = (z + dz) % RING_0 * RING_1 + (x + dx) % RING_1
            pairs.append((source, z * RING_1 + x))
    return lax.ppermute(array, ROWS, pairs)


def merge_kernel(tq, lq, hq, tk, lk, hk, tv, lv, hv, out):
    chunk = 0
    for train, low, high in ((tq, lq, hq), (tk, lk, hk), (tv, lv, hv)):
        result = train[...].astype(jnp.float32) + mix_rate * jnp.dot(
            low[...], high[...], preferred_element_type=jnp.float32
        )
        result = result.astype(jnp.bfloat16)
        for at in range(0, result.shape[1], LANES):
            out[chunk * BLOCK : (chunk + 1) * BLOCK, :] = result[:, at : at + LANES]
            chunk += 1
    out[WEIGHT_ROWS:, :] = jnp.zeros((SENT_ROWS - WEIGHT_ROWS, LANES), jnp.bfloat16)


def gain_kernel(_, own, first, second, third, out):
    out[WEIGHT_ROWS:, :] = own[...] + first[...] + second[...] + third[...]


def size_of(half):
    first, last = half
    return (last - first) * BLOCK + (SENT_ROWS - WEIGHT_ROWS if last == CHUNKS else 0)


def pack(sent, parts):
    total = sum(size for _, _, size in parts)
    if len({at for at, _, _ in parts}) == 1 and sent[parts[0][0]].shape[0] == total:
        return sent[parts[0][0]]
    used = sorted({at for at, _, _ in parts})

    def kernel(*refs):
        to = 0
        for at, row, size in parts:
            refs[-1][to : to + size, :] = refs[used.index(at)][row : row + size, :]
            to += size

    vmem = pl.BlockSpec(memory_space=pltpu.VMEM)
    return pl.pallas_call(
        kernel,
        out_shape=pltpu.VMEM((total, LANES), jnp.bfloat16),
        in_specs=[vmem] * len(used),
        out_specs=vmem,
        compiler_params=pltpu.CompilerParams(vmem_limit_bytes=2**20),
        name="pack",
    )(*(pltpu.with_memory_space_constraint(sent[at], pltpu.VMEM) for at in used))


def place_kernel(pieces, *refs):
    n = 1 + max(p[0] for p in pieces)
    sent, (query, key, value, norm), (rows, tiles, turned, sems) = refs[:n], refs[n : n + 4], refs[n + 4 :]
    z, x = lax.axis_index("rows_0"), lax.axis_index("rows_1")
    placed = []
    for at, row, (first, last), (dz, dx) in pieces:
        rank = lax.rem(z + dz, RING_0) * RING_1 + lax.rem(x + dx, RING_1)
        placed.append((sent[at], row, first, last, rank))
    copies = []
    for chunk in range(CHUNKS):
        for block, row, first, last, rank in placed:
            if first <= chunk < last:
                at = row + (chunk - first) * BLOCK
                rows[chunk, pl.ds(pl.multiple_of(rank * BLOCK, BLOCK), BLOCK), :] = block[at : at + BLOCK, :]
        for tile in range(RANKS * BLOCK // LANES):
            lanes = slice(tile * LANES, (tile + 1) * LANES)
            turned[chunk, :, lanes] = rows[chunk, lanes, :].T
        out, row = ((query, chunk), (key, chunk - 4), (value, chunk - 5))[max(0, chunk - 3)]
        copies.append(
            pltpu.make_async_copy(turned.at[chunk], out.at[row * LANES : (row + 1) * LANES, :], sems.at[chunk])
        )
        copies[-1].start()
    for block, row, first, last, rank in placed:
        if last == CHUNKS:
            at = row + (last - first) * BLOCK
            tiles[rank] = block[at : at + 8, :].astype(jnp.float32)
    lane = lax.broadcasted_iota(jnp.int32, (1, LANES), 1)
    for pair in range(RANKS // 2):
        both = jnp.where(lane < BLOCK, tiles[2 * pair, 0:1, :], tiles[2 * pair + 1, 0:1, :])
        norm[pair : pair + 1, :] = both.astype(jnp.bfloat16)
    for copy in copies:
        copy.wait()


def shards(
    train_query,
    low_query,
    high_query,
    train_key,
    low_key,
    high_key,
    train_value,
    low_value,
    high_value,
    norm_train,
    norm_step,
):
    bf16, vmem = jnp.bfloat16, pl.BlockSpec(memory_space=pltpu.VMEM)
    gain = jnp.tile((norm_train + norm_step).astype(bf16), LANES // 16)
    own = lax.broadcasted_iota(jnp.int32, (8, LANES), 1) // 16 % TP == lax.axis_index("tp")
    gain = jnp.where(own, gain[None, :], jnp.zeros((), bf16))
    others = [lax.ppermute(gain, "tp", [(i, (i + s) % TP) for i in range(TP)]) for s in range(1, TP)]
    block = pl.pallas_call(
        merge_kernel,
        out_shape=pltpu.VMEM((SENT_ROWS, LANES), bf16),
        in_specs=[vmem] * 9,
        out_specs=vmem,
        name="merge",
    )(train_query, low_query, high_query, train_key, low_key, high_key, train_value, low_value, high_value)
    block = pl.pallas_call(
        gain_kernel,
        out_shape=pltpu.VMEM((SENT_ROWS, LANES), bf16),
        in_specs=[vmem] * 5,
        out_specs=vmem,
        input_output_aliases={0: 0},
        name="gain",
    )(*(pltpu.with_memory_space_constraint(a, pltpu.VMEM) for a in (block, gain, *others)))

    sent = [block]
    held = {(0, 0, FIRST): (0, 0), (0, 0, LAST): (0, size_of(FIRST))}
    for offset, passed in STEPS:
        parts, row = [], 0
        for dz, dx, halves in passed:
            for half in halves:
                at, start = held[dz, dx, half]
                parts.append((at, start, size_of(half)))
                held[(offset[0] + dz) % RING_0, (offset[1] + dx) % RING_1, half] = (len(sent), row)
                row += size_of(half)
        sent.append(from_offset(pack(sent, parts), *offset))
    pieces = [(at, row, half, (dz, dx)) for (dz, dx, half), (at, row) in held.items()]
    assert len(pieces) == 2 * RANKS == 2 + sum(len(halves) for _, passed in STEPS for _, _, halves in passed)

    hbm = pl.BlockSpec(memory_space=pl.ANY)
    width = RANKS * BLOCK
    query, key, value, norm = pl.pallas_call(
        lambda *refs: place_kernel(pieces, *refs),
        out_shape=(
            jax.ShapeDtypeStruct((4 * LANES, width), bf16),
            jax.ShapeDtypeStruct((LANES, width), bf16),
            jax.ShapeDtypeStruct((LANES, width), bf16),
            jax.ShapeDtypeStruct((RANKS // 2, LANES), bf16),
        ),
        in_specs=[vmem] * len(sent),
        out_specs=(hbm, hbm, hbm, vmem),
        scratch_shapes=[
            pltpu.VMEM((CHUNKS, width, LANES), bf16),
            pltpu.VMEM((RANKS, 8, LANES), jnp.float32),
            pltpu.VMEM((CHUNKS, LANES, width), bf16),
            pltpu.SemaphoreType.DMA((CHUNKS,)),
        ],
        compiler_params=pltpu.CompilerParams(vmem_limit_bytes=16 * 2**20),
        name="place",
    )(*(pltpu.with_memory_space_constraint(a, pltpu.VMEM) for a in sent))
    return query, key, value, norm.reshape(width)


def solution(mesh):
    split = Mesh(
        mesh.devices.reshape(RING_0, RING_1, mesh.shape["tp"], mesh.shape["unit"]),
        ("rows_0", "rows_1", "tp", "unit"),
    )
    return jax.shard_map(
        shards,
        mesh=split,
        in_specs=(
            P(UNIT_ROWS, "tp"),
            P(UNIT_ROWS, None),
            P("unit", "tp"),
            P(UNIT_ROWS, "tp"),
            P(UNIT_ROWS, None),
            P("unit", "tp"),
            P(UNIT_ROWS, "tp"),
            P(UNIT_ROWS, None),
            P("unit", "tp"),
            P(UNIT_ROWS_TP),
            P(UNIT_ROWS_TP),
        ),
        out_specs=(
            P(("unit", "tp"), None),
            P(("unit", "tp"), None),
            P(("unit", "tp"), None),
            P("unit"),
        ),
        check_vma=False,
    )
```

```python
import jax
import jax.numpy as jnp
from jax import lax
from jax.experimental import pallas as pl
from jax.experimental.pallas import tpu as pltpu
from jax.sharding import Mesh
from jax.sharding import PartitionSpec as P

ROWS = ("rows_0", "rows_1")
UNIT_ROWS = ("unit", "rows_0", "rows_1")
UNIT_ROWS_TP = ("unit", "rows_0", "rows_1", "tp")
RING_0, RING_1, TP = 8, 4, 4
RANKS = RING_0 * RING_1

mix_rate = 0.5

LANES = 128
BLOCK = 64
CHUNKS = 6
WEIGHT_ROWS = CHUNKS * BLOCK
SENT_ROWS = WEIGHT_ROWS + 8

FIRST, LAST = (0, CHUNKS // 2), (CHUNKS // 2, CHUNKS)
WHOLE = (FIRST, LAST)
STEPS = (
    ((5, 0), ((0, 0, WHOLE),)),
    ((2, 2), ((0, 0, WHOLE),)),
    ((6, 2), ((0, 0, WHOLE),)),
    ((1, 0), ((0, 0, WHOLE),)),
    ((0, 1), ((0, 0, WHOLE),)),
    ((-1, 0), ((5, 0, WHOLE), (0, 0, WHOLE),)),
    ((0, -1), ((0, 0, WHOLE), (2, 2, WHOLE), (5, 0, WHOLE),)),
    ((1, 0), ((1, 0, WHOLE), (2, 2, WHOLE),)),
    ((0, 1), ((0, 1, WHOLE), (2, 2, WHOLE), (5, 0, WHOLE), (6, 2, WHOLE),)),
    ((-1, 0), ((2, 2, WHOLE), (4, 0, WHOLE), (6, 2, WHOLE), (7, 0, WHOLE), (0, 1, WHOLE),)),
    ((0, -1), ((1, 0, WHOLE), (4, 0, WHOLE), (6, 2, WHOLE), (7, 0, WHOLE),)),
    ((1, 0), ((0, 1, (LAST,)), (2, 1, WHOLE), (3, 2, WHOLE), (6, 2, WHOLE),)),
    ((0, 1), ((1, 0, (FIRST,)), (3, 2, WHOLE), (4, 0, WHOLE),)),
)


def from_offset(array, dz, dx):
    pairs = []
    for z in range(RING_0):
        for x in range(RING_1):
            source = (z + dz) % RING_0 * RING_1 + (x + dx) % RING_1
            pairs.append((source, z * RING_1 + x))
    return lax.ppermute(array, ROWS, pairs)


def merge_kernel(tq, lq, hq, tk, lk, hk, tv, lv, hv, out):
    chunk = 0
    for train, low, high in ((tq, lq, hq), (tk, lk, hk), (tv, lv, hv)):
        result = train[...].astype(jnp.float32) + mix_rate * jnp.dot(
            low[...], high[...], preferred_element_type=jnp.float32
        )
        result = result.astype(jnp.bfloat16)
        for at in range(0, result.shape[1], LANES):
            out[chunk * BLOCK : (chunk + 1) * BLOCK, :] = result[:, at : at + LANES]
            chunk += 1
    out[WEIGHT_ROWS:, :] = jnp.zeros((SENT_ROWS - WEIGHT_ROWS, LANES), jnp.bfloat16)


def gain_kernel(_, own, first, second, third, out):
    out[WEIGHT_ROWS:, :] = own[...] + first[...] + second[...] + third[...]


def size_of(half):
    first, last = half
    return (last - first) * BLOCK + (SENT_ROWS - WEIGHT_ROWS if last == CHUNKS else 0)


def pack(sent, parts):
    total = sum(size for _, _, size in parts)
    if len({at for at, _, _ in parts}) == 1 and sent[parts[0][0]].shape[0] == total:
        return sent[parts[0][0]]
    used = sorted({at for at, _, _ in parts})

    def kernel(*refs):
        to = 0
        for at, row, size in parts:
            refs[-1][to : to + size, :] = refs[used.index(at)][row : row + size, :]
            to += size

    vmem = pl.BlockSpec(memory_space=pltpu.VMEM)
    return pl.pallas_call(
        kernel,
        out_shape=pltpu.VMEM((total, LANES), jnp.bfloat16),
        in_specs=[vmem] * len(used),
        out_specs=vmem,
        compiler_params=pltpu.CompilerParams(vmem_limit_bytes=2**20),
        name="pack",
    )(*(pltpu.with_memory_space_constraint(sent[at], pltpu.VMEM) for at in used))


def place_kernel(pieces, *refs):
    n = 1 + max(p[0] for p in pieces)
    sent, (query, key, value, norm), (rows, tiles, turned, sems) = refs[:n], refs[n : n + 4], refs[n + 4 :]
    z, x = lax.axis_index("rows_0"), lax.axis_index("rows_1")
    placed = []
    for at, row, (first, last), (dz, dx) in pieces:
        rank = lax.rem(z + dz, RING_0) * RING_1 + lax.rem(x + dx, RING_1)
        placed.append((sent[at], row, first, last, rank))
    copies = []
    for chunk in range(CHUNKS):
        for block, row, first, last, rank in placed:
            if first <= chunk < last:
                at = row + (chunk - first) * BLOCK
                rows[chunk, pl.ds(pl.multiple_of(rank * BLOCK, BLOCK), BLOCK), :] = block[at : at + BLOCK, :]
        out, row = ((query, chunk), (key, chunk - 4), (value, chunk - 5))[max(0, chunk - 3)]
        half = RANKS * BLOCK // 2
        for part in range(2):
            for tile in range(half // LANES):
                lanes = slice(part * half + tile * LANES, part * half + (tile + 1) * LANES)
                turned[chunk, :, lanes] = rows[chunk, lanes, :].T
            lanes = slice(part * half, (part + 1) * half)
            copies.append(
                pltpu.make_async_copy(
                    turned.at[chunk, :, lanes],
                    out.at[row * LANES : (row + 1) * LANES, lanes],
                    sems.at[2 * chunk + part],
                )
            )
            copies[-1].start()
    for block, row, first, last, rank in placed:
        if last == CHUNKS:
            at = row + (last - first) * BLOCK
            tiles[rank] = block[at : at + 8, :].astype(jnp.float32)
    lane = lax.broadcasted_iota(jnp.int32, (1, LANES), 1)
    for pair in range(RANKS // 2):
        both = jnp.where(lane < BLOCK, tiles[2 * pair, 0:1, :], tiles[2 * pair + 1, 0:1, :])
        norm[pair : pair + 1, :] = both.astype(jnp.bfloat16)
    for copy in copies:
        copy.wait()


def shards(
    train_query,
    low_query,
    high_query,
    train_key,
    low_key,
    high_key,
    train_value,
    low_value,
    high_value,
    norm_train,
    norm_step,
):
    bf16, vmem = jnp.bfloat16, pl.BlockSpec(memory_space=pltpu.VMEM)
    gain = jnp.tile((norm_train + norm_step).astype(bf16), LANES // 16)
    own = lax.broadcasted_iota(jnp.int32, (8, LANES), 1) // 16 % TP == lax.axis_index("tp")
    gain = jnp.where(own, gain[None, :], jnp.zeros((), bf16))
    others = [lax.ppermute(gain, "tp", [(i, (i + s) % TP) for i in range(TP)]) for s in range(1, TP)]
    block = pl.pallas_call(
        merge_kernel,
        out_shape=pltpu.VMEM((SENT_ROWS, LANES), bf16),
        in_specs=[vmem] * 9,
        out_specs=vmem,
        name="merge",
    )(train_query, low_query, high_query, train_key, low_key, high_key, train_value, low_value, high_value)
    block = pl.pallas_call(
        gain_kernel,
        out_shape=pltpu.VMEM((SENT_ROWS, LANES), bf16),
        in_specs=[vmem] * 5,
        out_specs=vmem,
        input_output_aliases={0: 0},
        name="gain",
    )(*(pltpu.with_memory_space_constraint(a, pltpu.VMEM) for a in (block, gain, *others)))

    sent = [block]
    held = {(0, 0, FIRST): (0, 0), (0, 0, LAST): (0, size_of(FIRST))}
    for offset, passed in STEPS:
        parts, row = [], 0
        for dz, dx, halves in passed:
            for half in halves:
                at, start = held[dz, dx, half]
                parts.append((at, start, size_of(half)))
                held[(offset[0] + dz) % RING_0, (offset[1] + dx) % RING_1, half] = (len(sent), row)
                row += size_of(half)
        sent.append(from_offset(pack(sent, parts), *offset))
    pieces = [(at, row, half, (dz, dx)) for (dz, dx, half), (at, row) in held.items()]
    assert len(pieces) == 2 * RANKS == 2 + sum(len(halves) for _, passed in STEPS for _, _, halves in passed)

    hbm = pl.BlockSpec(memory_space=pl.ANY)
    width = RANKS * BLOCK
    query, key, value, norm = pl.pallas_call(
        lambda *refs: place_kernel(pieces, *refs),
        out_shape=(
            jax.ShapeDtypeStruct((4 * LANES, width), bf16),
            jax.ShapeDtypeStruct((LANES, width), bf16),
            jax.ShapeDtypeStruct((LANES, width), bf16),
            jax.ShapeDtypeStruct((RANKS // 2, LANES), bf16),
        ),
        in_specs=[vmem] * len(sent),
        out_specs=(hbm, hbm, hbm, vmem),
        scratch_shapes=[
            pltpu.VMEM((CHUNKS, width, LANES), bf16),
            pltpu.VMEM((RANKS, 8, LANES), jnp.float32),
            pltpu.VMEM((CHUNKS, LANES, width), bf16),
            pltpu.SemaphoreType.DMA((2 * CHUNKS,)),
        ],
        compiler_params=pltpu.CompilerParams(vmem_limit_bytes=16 * 2**20),
        name="place",
    )(*(pltpu.with_memory_space_constraint(a, pltpu.VMEM) for a in sent))
    return query, key, value, norm.reshape(width)


def solution(mesh):
    split = Mesh(
        mesh.devices.reshape(RING_0, RING_1, mesh.shape["tp"], mesh.shape["unit"]),
        ("rows_0", "rows_1", "tp", "unit"),
    )
    return jax.shard_map(
        shards,
        mesh=split,
        in_specs=(
            P(UNIT_ROWS, "tp"),
            P(UNIT_ROWS, None),
            P("unit", "tp"),
            P(UNIT_ROWS, "tp"),
            P(UNIT_ROWS, None),
            P("unit", "tp"),
            P(UNIT_ROWS, "tp"),
            P(UNIT_ROWS, None),
            P("unit", "tp"),
            P(UNIT_ROWS_TP),
            P(UNIT_ROWS_TP),
        ),
        out_specs=(
            P(("unit", "tp"), None),
            P(("unit", "tp"), None),
            P(("unit", "tp"), None),
            P("unit"),
        ),
        check_vma=False,
    )
```
